8 devices in a mesh: dp: 2 (over z, y), ep: 4 (over x, core).
Axes of the slice: x: 2, y: 2, z: 1, core: 2. Of those that a mesh axis runs over, the one named last changes fastest.
Arguments:
- hidden: bfloat16 [8192, 2048], P(('dp', 'ep'))
- grad_out: bfloat16 [8192, 2048], P(('dp', 'ep'))
- expert_ids: int32 [8192, 2], P(('dp', 'ep'))
- norm_gain: float32 [2048], replicated
- w_router: float32 [2048, 8], replicated
- w_gate: bfloat16 [8, 2048, 5632], P('ep')
- w_up: bfloat16 [8, 2048, 5632], P('ep')
- w_down: bfloat16 [8, 5632, 2048], P('ep')
Outputs:
- output 1: bfloat16 [8192, 2048], P(('dp', 'ep'))
- output 2: float32 [], replicated
- output 3: bfloat16 [8192, 2048], P(('dp', 'ep'))
- output 4: float32 [2048], replicated
- output 5: float32 [2048, 8], replicated
- output 6: bfloat16 [8, 2048, 5632], P('ep')
- output 7: bfloat16 [8, 2048, 5632], P('ep')
- output 8: bfloat16 [8, 5632, 2048], P('ep')
All inputs are finite; a program needn't handle non-finite values.
Results may differ from the reference program's by a relative error of at most 0.014439.
Values are sent between devices in bfloat16 or wider.
A program may use at most 1.25 GiB of HBM per device.

```python
import functools
import jax
import jax.numpy as jnp
from jax import lax

D = 2048
FF = 5632
EXPERTS = 8
TOK = 1024
DEVICES = 8
CAP = 4 * TOK // EXPERTS
ROWS_EXP = DEVICES * CAP
S_ALL = TOK * DEVICES
EPS = 1e-6
AUX_COEF = 0.001


def draw_routes(key):
    key_order, key_shift, key_perm, key_swap = jax.random.split(key, 4)
    half_exp = EXPERTS // 2
    mean_load = 2 * TOK // EXPERTS
    shift = jax.random.randint(key_shift, (DEVICES, half_exp), 0, mean_load + 1)
    shift = shift.at[:, 0].set(mean_load)
    order = jax.vmap(lambda sub_key: jax.random.permutation(sub_key, EXPERTS))(jax.random.split(key_order, DEVICES))
    signed = jnp.concatenate([shift, -shift], axis=1)
    expert_range = jnp.arange(EXPERTS, dtype=jnp.int32)
    loads = mean_load + jnp.sum(signed[:, :, None] * (order[:, :, None] == expert_range).astype(jnp.int32), axis=1)
    bounds = jnp.cumsum(loads, axis=1)
    positions = jnp.arange(2 * TOK, dtype=jnp.int32)
    listed = jax.vmap(lambda bound_row: jnp.searchsorted(bound_row, positions, side="right"))(bounds).astype(jnp.int32)
    token_order = jax.vmap(lambda sub_key: jax.random.permutation(sub_key, TOK))(jax.random.split(key_perm, DEVICES))
    first = jnp.take_along_axis(listed[:, :TOK], token_order, axis=1)
    second = jnp.take_along_axis(listed[:, TOK:], token_order, axis=1)
    swap = jax.random.randint(key_swap, (DEVICES, TOK), 0, 2) == 1
    id_first = jnp.where(swap, second, first)
    id_second = jnp.where(swap, first, second)
    return jnp.stack([id_first, id_second], axis=-1).reshape(DEVICES * TOK, 2).astype(jnp.int32)


def setup_inputs(seed: int = 0) -> dict:
    key = jax.random.key(seed)
    keys = jax.random.split(key, 8)
    expert_ids = draw_routes(keys[0])
    w_router = jax.random.normal(keys[1], (D, EXPERTS), jnp.float32) * D ** -0.5
    col_dir = w_router * lax.rsqrt(jnp.mean(w_router * w_router, axis=0, keepdims=True))
    chosen = jnp.sum((expert_ids[:, :, None] == jnp.arange(EXPERTS, dtype=jnp.int32)).astype(jnp.float32), axis=1)
    boost = jnp.dot(chosen, col_dir.T, preferred_element_type=jnp.float32)
    hidden = jax.random.normal(keys[2], (S_ALL, D), jnp.float32) + (2.5 * D ** -0.5) * boost
    grad_out = jax.random.normal(keys[3], (S_ALL, D), jnp.float32)
    norm_gain = 1.0 + 0.3 * jax.random.normal(keys[4], (D,), jnp.float32)
    w_gate = jax.random.normal(keys[5], (EXPERTS, D, FF), jnp.float32) * D ** -0.5
    w_up = jax.random.normal(keys[6], (EXPERTS, D, FF), jnp.float32) * D ** -0.5
    w_down = jax.random.normal(keys[7], (EXPERTS, FF, D), jnp.float32) * (2.0 * FF ** -0.5)
    return {"hidden": hidden.astype(jnp.bfloat16), "grad_out": grad_out.astype(jnp.bfloat16), "expert_ids": expert_ids, "norm_gain": norm_gain, "w_router": w_router, "w_gate": w_gate.astype(jnp.bfloat16), "w_up": w_up.astype(jnp.bfloat16), "w_down": w_down.astype(jnp.bfloat16)}


def bf16_trip(value):
    return value.astype(jnp.bfloat16).astype(jnp.float32)


def route_tables(expert_ids, n_exp, capacity):
    flat_ids = expert_ids.reshape(-1)
    n_choice = flat_ids.shape[0]
    one_hot = (flat_ids[:, None] == jnp.arange(n_exp, dtype=jnp.int32)[None, :]).astype(jnp.int32)
    running = jnp.cumsum(one_hot, axis=0) - 1
    dest_rows = flat_ids * capacity + jnp.sum(running * one_hot, axis=1)
    slot_owner = jnp.full((n_exp * capacity,), n_choice, jnp.int32).at[dest_rows].set(jnp.arange(n_choice, dtype=jnp.int32))
    return dest_rows, slot_owner, jnp.sum(one_hot, axis=0)


def expert_ffn(operands):
    rows, gate_w, up_w, down_w = operands
    h_gate = bf16_trip(jnp.dot(rows, gate_w.astype(jnp.float32), preferred_element_type=jnp.float32))
    h_up = bf16_trip(jnp.dot(rows, up_w.astype(jnp.float32), preferred_element_type=jnp.float32))
    act_rows = bf16_trip(jax.nn.silu(h_gate) * h_up)
    return bf16_trip(jnp.dot(act_rows, down_w.astype(jnp.float32), preferred_element_type=jnp.float32))


def forward_pass(hidden, norm_gain, w_router, w_gate, w_up, w_down, expert_ids):
    dest_rows, slot_owner, loads = route_tables(expert_ids, EXPERTS, ROWS_EXP)
    choice_hot = (expert_ids[:, :, None] == jnp.arange(EXPERTS, dtype=jnp.int32)).astype(jnp.float32)
    x_f32 = hidden.astype(jnp.float32)
    inv_rms = lax.rsqrt(jnp.mean(x_f32 * x_f32, axis=-1, keepdims=True) + EPS)
    x_norm = bf16_trip(x_f32 * inv_rms * norm_gain)
    logits = jnp.dot(x_norm, w_router, preferred_element_type=jnp.float32)
    router_probs = jax.nn.softmax(logits, axis=-1)
    gate_vals = jnp.sum(router_probs[:, None, :] * choice_hot, axis=-1)
    rows = bf16_trip(jnp.take(x_norm, slot_owner // 2, axis=0, mode="fill", fill_value=0))
    exp_out = lax.map(jax.checkpoint(expert_ffn), (rows.reshape(EXPERTS, ROWS_EXP, D), w_gate, w_up, w_down))
    picked = jnp.take(exp_out.reshape(EXPERTS * ROWS_EXP, D), dest_rows, axis=0).reshape(S_ALL, 2, D)
    out_hidden = (x_f32 + jnp.sum(gate_vals[:, :, None] * picked, axis=1)).astype(jnp.bfloat16)
    load_frac = loads.astype(jnp.float32) / (2 * S_ALL)
    aux_loss = AUX_COEF * EXPERTS * jnp.sum(load_frac * jnp.mean(router_probs, axis=0))
    return out_hidden, aux_loss


def reference(hidden, grad_out, expert_ids, norm_gain, w_router, w_gate, w_up, w_down):
    forward_fn = functools.partial(forward_pass, expert_ids=expert_ids)
    (out_hidden, aux_loss), pullback = jax.vjp(forward_fn, hidden, norm_gain, w_router, w_gate, w_up, w_down)
    all_grads = pullback((grad_out, jnp.ones_like(aux_loss)))
    return (out_hidden, aux_loss, all_grads[0], all_grads[1], all_grads[2], all_grads[3], all_grads[4], all_grads[5])
```

```python
import functools

import jax
import jax.numpy as jnp
from jax import lax
from jax.experimental import pallas as pl
from jax.experimental.pallas import tpu as pltpu
from jax.sharding import PartitionSpec as P

EPS = 1e-6
AUX_COEF = 0.001
GRP = 8
TILE = 512
STEP = 128
VMEM = 60 * 1024 * 1024


def dot(a, b, ca, cb):
    return lax.dot_general(a, b, (((ca,), (cb,)), ((), ())), preferred_element_type=jnp.float32)


def sized(need, tile, body):
    for k in range(1, tile // STEP + 1):
        pl.when(need == k)(functools.partial(body, k * STEP))


def tile_table(counts, stride, tile):
    per = stride // tile
    n_tiles = jnp.maximum((counts + tile - 1) // tile, 1)
    t = jnp.arange(2 * per, dtype=jnp.int32)
    expert = (t >= n_tiles[0]).astype(jnp.int32)
    i = t - expert * n_tiles[0]
    mine = jnp.where(expert == 0, counts[0], counts[1])
    last = jnp.where(expert == 0, n_tiles[0], n_tiles[1]) - 1
    rows = jnp.clip(mine - i * tile, 0, tile)
    block = jnp.minimum(expert * per + i, 2 * per - 1)
    steps = jnp.maximum((rows + STEP - 1) // STEP, 1)
    total = jnp.broadcast_to(n_tiles[0] + n_tiles[1], t.shape)
    return jnp.stack([expert, block, steps, (i == 0).astype(jnp.int32), (i == last).astype(jnp.int32), i * tile, rows, total])


def piped(name, body, grid, tables, ins, in_specs, outs, out_specs, scratch, flops, transcendentals=0):
    n_tab, n_in, n_out = len(tables), len(ins), len(outs)

    def kernel(*refs):
        tabs, in_refs, rest = refs[:n_tab], refs[n_tab : n_tab + n_in], refs[n_tab + n_in :]
        out_refs, scratch_refs = rest[:n_out], rest[n_out:]
        blocked = lambda specs: [pl.BlockSpec(shape, functools.partial(index, *tabs)) for shape, index in specs if shape]
        given = [r for r, (shape, _) in zip(in_refs, in_specs, strict=True) if shape]
        made = [r for r, (shape, _) in zip(out_refs, out_specs, strict=True) if shape]
        plain = [r for r, (shape, _) in zip(out_refs, out_specs, strict=True) if not shape]
        step = lambda *blocks: body(*tabs, *blocks, *plain, *scratch_refs)
        pltpu.emit_pipeline(step, grid=grid(*tabs), in_specs=blocked(in_specs), out_specs=blocked(out_specs))(*given, *made)

    size = lambda v: v.size * v.dtype.itemsize
    return pl.pallas_call(
        kernel,
        in_specs=[pl.BlockSpec(memory_space=pltpu.SMEM)] * n_tab + [pl.BlockSpec(memory_space=pltpu.HBM)] * n_in,
        out_specs=[pl.BlockSpec(memory_space=pltpu.HBM)] * n_out,
        out_shape=outs,
        scratch_shapes=scratch,
        compiler_params=pltpu.CompilerParams(vmem_limit_bytes=VMEM),
        cost_estimate=pl.CostEstimate(flops=flops, bytes_accessed=sum(map(size, [*ins, *outs])), transcendentals=transcendentals),
        name=name,
    )(*tables, *ins)


def sigmoid(v):
    return 0.5 * jnp.tanh(0.5 * v) + 0.5


def route_kernel(scaled, order, offs, lens, ends, tok_ref, rows_ref, gate_ref, out_ref, buf, zero, sem, zsem):
    p, l = pl.program_id(0), pl.program_id(1)
    n_l = pl.num_programs(1)
    at = p * n_l + l
    slot = lax.rem(at, 2)

    def copy(i, where):
        n = lens[i]
        return pltpu.make_async_copy(buf.at[where, pl.ds(0, n)], out_ref.at[pl.ds(offs[i], n)], sem.at[where])

    @pl.when((at >= 2) & (lens[jnp.maximum(at - 2, 0)] > 0))
    def _():
        copy(at - 2, slot).wait()

    n_tok, width = tok_ref.shape

    def body(rows):
        idx = rows_ref[0, 0, :, :rows]
        pick = (lax.broadcasted_iota(jnp.int32, (n_tok, rows), 0) == idx).astype(jnp.float32).astype(jnp.bfloat16)
        got = dot(pick, tok_ref[...], 0, 0)
        if scaled:
            got = got * gate_ref[0, 0, :rows, :]
        buf[slot, : rows // GRP] = got.reshape(rows // GRP, GRP, width).astype(jnp.bfloat16)

    sized((lens[at] * GRP + STEP - 1) // STEP, rows_ref.shape[3], body)

    @pl.when(lens[at] > 0)
    def _():
        copy(at, slot).start()

    @pl.when(at == n_l * pl.num_programs(0) - 1)
    def _():
        zero[...] = jnp.zeros_like(zero)
        for i in range(2):
            pltpu.make_async_copy(zero, out_ref.at[pl.ds(ends[i], zero.shape[0])], zsem).start()
        for i in range(2):
            pltpu.make_async_copy(zero, out_ref.at[pl.ds(ends[i], zero.shape[0])], zsem).wait()
        pl.when(lens[at - 1] > 0)(lambda: copy(at - 1, 1 - slot).wait())
        pl.when(lens[at] > 0)(lambda: copy(at, slot).wait())


def route_call(name, tokens, slot_rows, slot_gates, order, offs, lens, ends, n_tok, groups, scaled):
    width = tokens.shape[1]
    n_src, _, _, capacity = slot_rows.shape
    return piped(
        name,
        functools.partial(route_kernel, scaled),
        lambda *_: (n_src, 2),
        [order, offs, lens, ends],
        [tokens, slot_rows, slot_gates],
        [
            ((n_tok, width), lambda order, offs, lens, ends, p, l: (order[p], 0)),
            ((1, 1, 1, capacity), lambda order, offs, lens, ends, p, l: (order[p], l, 0, 0)),
            ((1, 1, capacity, 1), lambda order, offs, lens, ends, p, l: (order[p], l, 0, 0)),
        ],
        [jax.ShapeDtypeStruct((groups, GRP, width), jnp.bfloat16)],
        [(None, None)],
        [
            pltpu.VMEM((2, capacity // GRP, GRP, width), jnp.bfloat16),
            pltpu.VMEM((STEP // GRP, GRP, width), jnp.bfloat16),
            pltpu.SemaphoreType.DMA((2,)),
            pltpu.SemaphoreType.DMA,
        ],
        2 * n_src * capacity * n_tok * width,
    )[0]


def up_kernel(tab, x_ref, wg_ref, wu_ref, hg_ref, hu_ref, act_ref):
    t = pl.program_id(1)

    def body(rows):
        x = x_ref[:rows, :]
        hg = dot(x, wg_ref[0], 1, 0).astype(jnp.bfloat16)
        hu = dot(x, wu_ref[0], 1, 0).astype(jnp.bfloat16)
        gate = hg.astype(jnp.float32)
        hg_ref[:rows, :] = hg
        hu_ref[:rows, :] = hu
        act_ref[:rows, :] = (gate * sigmoid(gate) * hu.astype(jnp.float32)).astype(jnp.bfloat16)

    sized(tab[2, t], x_ref.shape[0], body)


def up_call(x, w_gate, w_up, table, fb, tile):
    rows, width = x.shape
    ff = w_gate.shape[2]
    w_in = ((1, width, fb), lambda tab, n, t: (tab[0, t], 0, n))
    out = ((tile, fb), lambda tab, n, t: (tab[1, t], n))
    return piped(
        "up",
        up_kernel,
        lambda tab: (ff // fb, tab[7, 0]),
        [table],
        [x, w_gate, w_up],
        [((tile, width), lambda tab, n, t: (tab[1, t], 0)), w_in, w_in],
        [jax.ShapeDtypeStruct((rows, ff), jnp.bfloat16)] * 3,
        [out] * 3,
        [],
        2 * rows * width * ff,
        rows * ff // 2,
    )


def down_kernel(n_in, tab, offs, lens, *refs):
    a_refs, w_refs, out_ref, buf, sem = refs[:n_in], refs[n_in : 2 * n_in], *refs[2 * n_in :]
    n, t = pl.program_id(0), pl.program_id(1)
    n_t = pl.num_programs(1)
    at = n * n_t + t
    slot = lax.rem(at, 2)
    tile, cols = a_refs[0].shape[0], buf.shape[3]
    n_src = lens.shape[1]

    def landed(tile_at, where):
        size = tab[6, tile_at] // GRP

        @pl.when(size > 0)
        def _():
            pltpu.make_async_copy(buf.at[where, pl.ds(0, size)], buf.at[where, pl.ds(0, size)], sem.at[where]).wait()

    @pl.when(at >= 2)
    def _():
        landed(lax.rem(at - 2, n_t), slot)

    def body(rows):
        total = dot(a_refs[0][:rows, :], w_refs[0][0], 1, 0 if n_in == 1 else 1)
        if n_in == 2:
            total = total + dot(a_refs[1][:rows, :], w_refs[1][0], 1, 1)
        buf[slot, : rows // GRP] = total.reshape(rows // GRP, GRP, cols).astype(jnp.bfloat16)

    sized(tab[2, t], tile, body)
    expert = tab[0, t]
    low = tab[5, t] // GRP
    high = low + tab[6, t] // GRP
    for s in range(n_src):
        start = jnp.maximum(offs[expert, s], low)
        size = jnp.minimum(offs[expert, s] + lens[expert, s], high) - start

        @pl.when(size > 0)
        def _():
            dst = out_ref.at[s, expert, pl.ds(start - offs[expert, s], size), :, pl.ds(pl.multiple_of(n * cols, cols), cols)]
            pltpu.make_async_copy(buf.at[slot, pl.ds(start - low, size)], dst, sem.at[slot]).start()

    @pl.when(at == n_t * pl.num_programs(0) - 1)
    def _():
        landed(t, slot)

        @pl.when(at >= 1)
        def _():
            landed(lax.rem(at - 1 + n_t, n_t), 1 - slot)


def down_call(name, acts, weights, table, offs, lens, capacity, cols, tile):
    ff = acts[0].shape[1]
    k = len(acts)
    width = weights[0].shape[2] if k == 1 else weights[0].shape[1]
    n_src = lens.shape[1]
    a_in = ((tile, ff), lambda tab, offs, lens, n, t: (tab[1, t], 0))
    if k == 1:
        w_in = ((1, ff, cols), lambda tab, offs, lens, n, t: (tab[0, t], 0, n))
    else:
        w_in = ((1, cols, ff), lambda tab, offs, lens, n, t: (tab[0, t], n, 0))
    return piped(
        name,
        functools.partial(down_kernel, k),
        lambda tab, offs, lens: (width // cols, tab[7, 0]),
        [table, offs, lens],
        [*acts, *weights],
        [a_in] * k + [w_in] * k,
        [jax.ShapeDtypeStruct((n_src, 2, capacity // GRP, GRP, width), jnp.bfloat16)],
        [(None, None)],
        [pltpu.VMEM((2, tile // GRP, GRP, cols), jnp.bfloat16), pltpu.SemaphoreType.DMA((2,))],
        k * n_src * capacity * 2 * width * ff,
    )[0]


def dact_kernel(tab, d_ref, w_ref, hg_ref, hu_ref, dg_ref, du_ref):
    t = pl.program_id(1)

    def body(rows):
        d_act = dot(d_ref[:rows, :], w_ref[0], 1, 1).astype(jnp.bfloat16).astype(jnp.float32)
        gate = hg_ref[:rows, :].astype(jnp.float32)
        up = hu_ref[:rows, :].astype(jnp.float32)
        sig = sigmoid(gate)
        silu = gate * sig
        du_ref[:rows, :] = (d_act * silu).astype(jnp.bfloat16)
        dg_ref[:rows, :] = (d_act * up * (sig + silu * (1.0 - sig))).astype(jnp.bfloat16)

    sized(tab[2, t], d_ref.shape[0], body)


def dact_call(d_out, w_down, h_gate, h_up, table, fb, tile):
    rows, width = d_out.shape
    ff = w_down.shape[1]
    h_blk = ((tile, fb), lambda tab, n, t: (tab[1, t], n))
    return piped(
        "dact",
        dact_kernel,
        lambda tab: (ff // fb, tab[7, 0]),
        [table],
        [d_out, w_down, h_gate, h_up],
        [((tile, width), lambda tab, n, t: (tab[1, t], 0)), ((1, fb, width), lambda tab, n, t: (tab[0, t], n, 0)), h_blk, h_blk],
        [jax.ShapeDtypeStruct((rows, ff), jnp.bfloat16)] * 2,
        [h_blk] * 2,
        [],
        rows * width * ff,
        rows * ff // 2,
    )


def wgrad_kernel(tab, x_ref, d_ref, dg_ref, du_ref, act_ref, gg_ref, gu_ref, gd_ref, ag_ref, au_ref, ad_ref):
    t = pl.program_id(1)
    first, last = tab[3, t] == 1, tab[4, t] == 1

    def products(rows):
        x = x_ref[:rows, :]
        yield ag_ref, gg_ref, dot(x, dg_ref[:rows, :], 0, 0)
        yield au_ref, gu_ref, dot(x, du_ref[:rows, :], 0, 0)
        yield ad_ref, gd_ref, dot(act_ref[:rows, :], d_ref[:rows, :], 0, 0)

    @pl.when(first & last)
    def _():
        for acc_ref in (ag_ref, au_ref, ad_ref):
            acc_ref[...] = jnp.zeros_like(acc_ref)

    @pl.when(first & ~last)
    def _():
        for acc_ref, _, part in products(x_ref.shape[0]):
            acc_ref[...] = part

    @pl.when(~first & ~last)
    def _():
        for acc_ref, _, part in products(x_ref.shape[0]):
            acc_ref[...] += part

    def finish(rows):
        for acc_ref, out_ref, part in products(rows):
            out_ref[0] = (acc_ref[...] + part).astype(jnp.bfloat16)

    sized(jnp.where(last, tab[2, t], 0), x_ref.shape[0], finish)


def wgrad_call(x, d_out, d_gate, d_up, act, table, fb, tile):
    rows, width = x.shape
    ff = act.shape[1]
    row_in = ((tile, width), lambda tab, n, t: (tab[1, t], 0))
    h_in = ((tile, fb), lambda tab, n, t: (tab[1, t], n))
    up_out = ((1, width, fb), lambda tab, n, t: (tab[0, t], 0, n))
    down_out = ((1, fb, width), lambda tab, n, t: (tab[0, t], n, 0))
    up_shape = jax.ShapeDtypeStruct((2, width, ff), jnp.bfloat16)
    down_shape = jax.ShapeDtypeStruct((2, ff, width), jnp.bfloat16)
    return piped(
        "wgrad",
        wgrad_kernel,
        lambda tab: (ff // fb, tab[7, 0]),
        [table],
        [x, d_out, d_gate, d_up, act],
        [row_in, row_in, h_in, h_in, h_in],
        [up_shape, up_shape, down_shape],
        [up_out, up_out, down_out],
        [pltpu.VMEM((width, fb), jnp.float32)] * 2 + [pltpu.VMEM((fb, width), jnp.float32)],
        3 * rows * width * ff,
    )


def excl(v, axis):
    return jnp.cumsum(v, axis=axis) - v


def solution(mesh):
    n_dp, n_ep = mesh.shape["dp"], mesh.shape["ep"]
    n_dev = n_dp * n_ep
    all_axes = ("dp", "ep")

    def local_step(hidden, grad_out, expert_ids, norm_gain, w_router, w_gate, w_up, w_down):
        n_tok, width = hidden.shape
        n_exp = w_router.shape[1]
        ff = w_gate.shape[2]
        capacity = 4 * n_tok // n_exp
        total_tok = n_tok * n_dev
        tile = min(TILE, capacity)
        fb = min(512, ff)
        cols = min(512, width)
        stride = n_dev * capacity + tile
        groups = 2 * stride // GRP
        dp, ep = lax.axis_index("dp"), lax.axis_index("ep")
        experts = jnp.arange(n_exp, dtype=jnp.int32)

        x_f32 = hidden.astype(jnp.float32)
        inv_rms = lax.rsqrt(jnp.mean(x_f32 * x_f32, axis=-1, keepdims=True) + EPS)
        x_hat = x_f32 * inv_rms
        x_norm = (x_hat * norm_gain).astype(jnp.bfloat16)
        all_tokens = lax.all_gather(x_norm, all_axes, axis=0, tiled=True)
        xn_f32 = x_norm.astype(jnp.float32)
        router_probs = jax.nn.softmax(jnp.dot(xn_f32, w_router, preferred_element_type=jnp.float32), axis=-1)
        choice_hot = (expert_ids[:, :, None] == experts).astype(jnp.float32)
        gate_vals = jnp.sum(router_probs[:, None, :] * choice_hot, axis=-1)

        flat_ids = expert_ids.reshape(-1)
        one_hot = (flat_ids[:, None] == experts[None, :]).astype(jnp.int32)
        running = jnp.cumsum(one_hot, axis=0) - 1
        dest_rows = flat_ids * capacity + jnp.sum(running * one_hot, axis=1)
        slots = jnp.arange(n_exp * capacity, dtype=jnp.int32)
        choices = jnp.arange(2 * n_tok, dtype=jnp.int32)
        hit = dest_rows[None, :] == slots[:, None]
        slot_tok = jnp.sum(jnp.where(hit, choices[None, :] // 2 + 1, 0), axis=1) - 1
        slot_gate = jnp.sum(jnp.where(hit, gate_vals.reshape(-1)[None, :], 0.0), axis=1)
        packed = jnp.stack([slot_tok.astype(jnp.float32), slot_gate]).reshape(2, n_exp, capacity)
        packed = lax.all_gather(packed, all_axes, axis=0, tiled=False)
        packed, late_out = lax.optimization_barrier((packed, grad_out))
        all_dy = lax.all_gather(late_out, all_axes, axis=0, tiled=True)
        all_toks = packed[:, 0].astype(jnp.int32)
        all_loads = jnp.sum((all_toks >= 0).astype(jnp.int32), axis=2)
        src_groups = (all_loads + GRP - 1) // GRP
        mine = lambda v: lax.dynamic_slice_in_dim(v, 2 * ep, 2, axis=1)
        order = lax.rem(jnp.arange(n_dev, dtype=jnp.int32) + dp * n_ep, n_dev)
        seg_len = jnp.take(mine(src_groups), order, axis=0)
        seg_off = excl(seg_len, 0)
        base = jnp.arange(2, dtype=jnp.int32) * (stride // GRP)
        n_all = jnp.sum(seg_len, axis=0)
        own_len, own_off = seg_len[:n_ep].T, seg_off[:n_ep].T
        tab_all = tile_table(n_all * GRP, stride, tile)
        tab_own = tile_table(jnp.sum(own_len, axis=1) * GRP, stride, tile)
        my_toks = mine(all_toks)[:, :, None, :]
        my_gates = mine(packed[:, 1])[:, :, :, None]
        route = functools.partial(
            route_call, slot_rows=my_toks, slot_gates=my_gates, order=order, offs=(seg_off + base).reshape(-1), lens=seg_len.reshape(-1), ends=n_all + base, n_tok=n_tok, groups=groups
        )

        x_rows = route("route", all_tokens, scaled=False).reshape(2 * stride, width)
        h_gate, h_up, act = up_call(x_rows, w_gate, w_up, tab_all, fb, tile)

        def send_back(blocks):
            return lax.all_to_all(blocks, "ep", 0, 0, tiled=True).reshape(n_exp * capacity, width)

        back = send_back(down_call("down", [act], [w_down], tab_own, own_off, own_len, capacity, cols, tile))
        d_rows = route("droute", all_dy, scaled=True).reshape(2 * stride, width)
        d_gate, d_up = dact_call(d_rows, w_down, h_gate, h_up, tab_all, fb, tile)
        d_blocks = down_call("drows", [d_gate, d_up], [w_gate, w_up], tab_own, own_off, own_len, capacity, cols, tile)
        back, d_blocks = lax.optimization_barrier((back, d_blocks))
        d_back = send_back(d_blocks)
        g_gate, g_up, g_down = wgrad_call(x_rows, d_rows, d_gate, d_up, act, tab_all, fb, tile)

        dest = dest_rows.reshape(n_tok, 2)
        pick = lambda rows, j: jnp.take(rows, dest[:, j], axis=0, mode="clip").astype(jnp.float32)
        dy_f32 = grad_out.astype(jnp.float32)
        out0, out1 = pick(back, 0), pick(back, 1)
        out_hidden = (x_f32 + (gate_vals[:, :1] * out0 + gate_vals[:, 1:] * out1)).astype(jnp.bfloat16)
        d_gates = jnp.stack([jnp.sum(dy_f32 * out0, axis=-1), jnp.sum(dy_f32 * out1, axis=-1)], axis=1)
        load_frac = jnp.sum(all_loads, axis=0).astype(jnp.float32) / (2 * total_tok)
        d_probs = jnp.sum(d_gates[:, :, None] * choice_hot, axis=1) + (AUX_COEF * n_exp / total_tok) * load_frac
        d_logits = router_probs * (d_probs - jnp.sum(router_probs * d_probs, axis=-1, keepdims=True))
        d_xnorm = jnp.einsum("te,de->td", d_logits, w_router) + pick(d_back, 0) + pick(d_back, 1)
        d_xnorm = d_xnorm.astype(jnp.bfloat16).astype(jnp.float32)
        d_hat = d_xnorm * norm_gain
        grad_hidden = (inv_rms * (d_hat - x_hat * jnp.mean(d_hat * x_hat, axis=-1, keepdims=True)) + dy_f32).astype(jnp.bfloat16)
        prob_sum, grad_gain, grad_router = lax.psum(
            (jnp.sum(router_probs, axis=0), jnp.sum(d_xnorm * x_hat, axis=0), jnp.einsum("td,te->de", xn_f32, d_logits)), all_axes
        )
        aux_loss = AUX_COEF * n_exp * jnp.sum(load_frac * prob_sum / total_tok)
        return out_hidden, aux_loss, grad_hidden, grad_gain, grad_router, g_gate, g_up, g_down

    tok_spec = P(all_axes, None)
    w_spec = P("ep", None, None)
    return jax.shard_map(
        local_step,
        mesh=mesh,
        in_specs=(tok_spec, tok_spec, tok_spec, P(), P(), w_spec, w_spec, w_spec),
        out_specs=(tok_spec, P(), tok_spec, P(), P(), w_spec, w_spec, w_spec),
        check_vma=False,
    )
```

```python
import functools

import jax
import jax.numpy as jnp
from jax import lax
from jax.experimental import pallas as pl
from jax.experimental.pallas import tpu as pltpu
from jax.sharding import PartitionSpec as P

EPS = 1e-6
AUX_COEF = 0.001
GRP = 8
UNIT = 128
VMEM = 62 * 1024 * 1024
I32 = jnp.int32


def dot(a, b, ca, cb):
    return lax.dot_general(a, b, (((ca,), (cb,)), ((), ())), preferred_element_type=jnp.float32)


def sigmoid(v):
    return 0.5 * jnp.tanh(0.5 * v) + 0.5


def rows_of(ref, start, rows):
    return ref.at[pl.ds(start, rows // GRP)].reshape(rows, ref.shape[2])


def grouped(value):
    rows, cols = value.shape
    return value.reshape(rows // GRP, GRP, cols).astype(jnp.bfloat16)


def units(groups):
    return (groups * GRP + UNIT - 1) // UNIT


def in_blocks(groups, largest, body):
    left = units(groups)
    per = largest // UNIT
    n_big = left // per
    step = UNIT // GRP

    def big(i, carry):
        body(pl.multiple_of(i * (per * step), per * step), largest)
        return carry

    lax.fori_loop(0, n_big, big, 0)
    start = n_big * per
    while per > 1:
        per //= 2
        take = (left & per) > 0
        pl.when(take)(functools.partial(body, pl.multiple_of(start * step, step), per * UNIT))
        start = start + jnp.where(take, per, 0)


def sized(need, most, body):
    for k in range(1, most // UNIT + 1):
        pl.when(need == k)(functools.partial(body, k * UNIT))


def piped(name, body, grid, tables, ins, in_specs, outs, out_specs, scratch, flops, transcendentals=0, into=()):
    n_tab, n_in, n_out, n_into = len(tables), len(ins), len(outs), len(into)

    def kernel(*refs):
        tabs, in_refs, rest = refs[:n_tab], refs[n_tab : n_tab + n_in], refs[n_tab + n_in + n_into :]
        out_refs, scratch_refs = rest[:n_out], rest[n_out:]
        blocked = lambda specs: [pl.BlockSpec(shape, functools.partial(index, *tabs)) for shape, index in specs if shape]
        given = [r for r, (shape, _) in zip(in_refs, in_specs, strict=True) if shape]
        made = [r for r, (shape, _) in zip(out_refs, out_specs, strict=True) if shape]
        plain = [r for r, (shape, _) in zip(out_refs, out_specs, strict=True) if not shape]
        step = lambda *blocks: body(*tabs, *blocks, *plain, *scratch_refs)
        pltpu.emit_pipeline(step, grid=grid(*tabs), in_specs=blocked(in_specs), out_specs=blocked(out_specs))(*given, *made)

    size = lambda v: v.size * v.dtype.itemsize
    hbm = pl.BlockSpec(memory_space=pltpu.HBM)
    return pl.pallas_call(
        kernel,
        in_specs=[pl.BlockSpec(memory_space=pltpu.SMEM)] * n_tab + [hbm] * (n_in + n_into),
        out_specs=[hbm] * n_out,
        out_shape=outs,
        scratch_shapes=scratch,
        input_output_aliases={n_tab + n_in + i: i for i in range(n_into)},
        compiler_params=pltpu.CompilerParams(vmem_limit_bytes=VMEM),
        cost_estimate=pl.CostEstimate(flops=flops, bytes_accessed=sum(map(size, [*ins, *outs])), transcendentals=transcendentals),
        name=name,
    )(*tables, *ins, *into)


def tile_rows(groups):
    return pl.BoundedSlice(groups)


def route_kernel(scaled, offs, lens, tok_ref, rows_ref, gate_ref, out_ref, buf, sem):
    p, l = pl.program_id(0), pl.program_id(1)
    n_src, n_l = pl.num_programs(0), pl.num_programs(1)
    at = p * n_l + l
    slot = lax.rem(at, 2)

    def copy(i, where):
        n = lens[i]
        return pltpu.make_async_copy(buf.at[where, pl.ds(0, n)], out_ref.at[pl.ds(offs[i], n)], sem.at[where])

    @pl.when((at >= 2) & (lens[jnp.maximum(at - 2, 0)] > 0))
    def _():
        copy(at - 2, slot).wait()

    n_tok, width = tok_ref.shape

    def body(rows):
        idx = rows_ref[0, 0, :, :rows]
        pick = (lax.broadcasted_iota(I32, (n_tok, rows), 0) == idx).astype(jnp.float32).astype(jnp.bfloat16)
        got = dot(pick, tok_ref[...], 0, 0)
        if scaled:
            got = got * gate_ref[0, 0, :rows, :]
        buf[slot, : rows // GRP] = grouped(got)

    sized(units(lens[at]), rows_ref.shape[3], body)

    @pl.when(lens[at] > 0)
    def _():
        copy(at, slot).start()

    @pl.when(at == n_l * n_src - 1)
    def _():
        pl.when(lens[at - 1] > 0)(lambda: copy(at - 1, 1 - slot).wait())
        pl.when(lens[at] > 0)(lambda: copy(at, slot).wait())


def route_call(name, tokens, slot_rows, slot_gates, offs, lens, n_tok, groups, scaled, into=()):
    width = tokens.shape[1]
    n_src, _, _, capacity = slot_rows.shape
    return piped(
        name,
        functools.partial(route_kernel, scaled),
        lambda *_: (n_src, 2),
        [offs, lens],
        [tokens, slot_rows, slot_gates],
        [
            ((n_tok, width), lambda offs, lens, p, l: (p, 0)),
            ((1, 1, 1, capacity), lambda offs, lens, p, l: (p, l, 0, 0)),
            ((1, 1, capacity, 1), lambda offs, lens, p, l: (p, l, 0, 0)),
        ],
        [jax.ShapeDtypeStruct((groups, GRP, width), jnp.bfloat16)],
        [(None, None)],
        [pltpu.VMEM((2, capacity // GRP, GRP, width), jnp.bfloat16), pltpu.SemaphoreType.DMA((2,))],
        2 * n_src * capacity * n_tok * width,
        into=into,
    )[0]


def up_kernel(tab, x_ref, wg_ref, wu_ref, hg_ref, hu_ref, act_ref):
    t = pl.program_id(0)

    def body(start, rows):
        part = min(rows, 512)
        for i in range(rows // part):
            at = start + i * (part // GRP)
            x = rows_of(x_ref, at, part)[...]
            hg = dot(x, wg_ref[0], 1, 0).astype(jnp.bfloat16)
            hu = dot(x, wu_ref[0], 1, 0).astype(jnp.bfloat16)
            gate = hg.astype(jnp.float32)
            to = pl.ds(at, part // GRP)
            hg_ref[to] = grouped(hg)
            hu_ref[to] = grouped(hu)
            act_ref[to] = grouped(gate * sigmoid(gate) * hu.astype(jnp.float32))

    in_blocks(tab[2, t], 1024, body)


def up_call(name, x, w_gate, w_up, table, fb, most, into=()):
    groups, _, width = x.shape
    ff = w_gate.shape[2]
    rows = lambda tab, t: pl.ds(tab[1, t], tab[2, t])
    w_in = ((1, width, fb), lambda tab, t, n: (tab[0, t], 0, n))
    out = ((tile_rows(most), GRP, fb), lambda tab, t, n: (rows(tab, t), 0, n))
    return piped(
        name,
        up_kernel,
        lambda tab: (table.shape[1], ff // fb),
        [table],
        [x, w_gate, w_up],
        [((tile_rows(most), GRP, width), lambda tab, t, n: (rows(tab, t), 0, 0)), w_in, w_in],
        [jax.ShapeDtypeStruct((groups, GRP, ff), jnp.bfloat16)] * 3,
        [out] * 3,
        [],
        groups * GRP * width * ff,
        groups * GRP * ff // 4,
        into=into,
    )


def down_kernel(k_in, tab, offs, lens, *refs):
    a_refs, w_refs, out_ref, acc_ref, buf, sem = refs[:k_in], refs[k_in : 2 * k_in], *refs[2 * k_in :]
    t, k = pl.program_id(0), pl.program_id(1)
    n_t, n_k = pl.num_programs(0), pl.num_programs(1)
    n_src = lens.shape[1]

    def body(start, rows):
        a = jnp.concatenate([rows_of(r, start, rows)[...] for r in a_refs], axis=1)
        if k_in == 1:
            part = dot(a, w_refs[0][0], 1, 0)
        else:
            part = dot(a, jnp.concatenate([w_refs[0][0], w_refs[1][0]], axis=1), 1, 1)
        to = pl.ds(pl.multiple_of(start * GRP, UNIT), rows)
        acc_ref[to, :] = jnp.where(k == 0, 0.0, acc_ref[to, :]) + part

    in_blocks(tab[2, t], 512, body)

    def landed(expert):
        size = tab[3, expert]

        @pl.when(size > 0)
        def _():
            pltpu.make_async_copy(buf.at[pl.ds(0, size)], buf.at[pl.ds(0, size)], sem).wait()

    @pl.when(k == n_k - 1)
    def _():
        pl.when(t > 0)(functools.partial(landed, t - 1))

        def flush(start, rows):
            buf[pl.ds(start, rows // GRP)] = grouped(acc_ref[pl.ds(pl.multiple_of(start * GRP, UNIT), rows), :])

        in_blocks(tab[2, t], UNIT, flush)
        for s in range(n_src):
            size = lens[t, s]

            @pl.when(size > 0)
            def _():
                pltpu.make_async_copy(buf.at[pl.ds(offs[t, s], size)], out_ref.at[s, t, pl.ds(0, size)], sem).start()

        pl.when(t == n_t - 1)(functools.partial(landed, t))


def down_call(name, acts, weights, table, offs, lens, capacity, kb, most):
    ff = acts[0].shape[2]
    k = len(acts)
    width = weights[0].shape[2] if k == 1 else weights[0].shape[1]
    n_src = lens.shape[1]
    a_in = ((tile_rows(most), GRP, kb), lambda tab, offs, lens, t, k: (pl.ds(tab[1, t], tab[2, t]), 0, k))
    if k == 1:
        w_in = ((1, kb, width), lambda tab, offs, lens, t, k: (tab[0, t], k, 0))
    else:
        w_in = ((1, width, kb), lambda tab, offs, lens, t, k: (tab[0, t], 0, k))
    return piped(
        name,
        functools.partial(down_kernel, k),
        lambda tab, offs, lens: (2, ff // kb),
        [table, offs, lens],
        [*acts, *weights],
        [a_in] * k + [w_in] * k,
        [jax.ShapeDtypeStruct((n_src, 2, capacity // GRP, GRP, width), jnp.bfloat16)],
        [(None, None)],
        [pltpu.VMEM((most * GRP, width), jnp.float32), pltpu.VMEM((most, GRP, width), jnp.bfloat16), pltpu.SemaphoreType.DMA],
        k * n_src * capacity * 2 * width * ff,
    )[0]


def dact_kernel(tab, d_ref, w_ref, hg_ref, hu_ref, dg_ref, du_ref, kept):
    t = pl.program_id(0)
    chunk = kept.shape[0]
    per = chunk // UNIT
    whole = (units(tab[2, t]) - 1) // per

    def product(at, rows):
        kept[:rows, :] = dot(rows_of(d_ref, at, rows)[...], w_ref[0], 1, 1).astype(jnp.bfloat16)

    def pointwise(at, rows):
        d_act = kept[:rows, :].astype(jnp.float32)
        gate = rows_of(hg_ref, at, rows)[...].astype(jnp.float32)
        up = rows_of(hu_ref, at, rows)[...].astype(jnp.float32)
        sig = sigmoid(gate)
        silu = gate * sig
        to = pl.ds(at, rows // GRP)
        du_ref[to] = grouped(d_act * silu)
        dg_ref[to] = grouped(d_act * up * (sig + silu * (1.0 - sig)))

    def at(c):
        return pl.multiple_of(c * (chunk // GRP), chunk // GRP)

    def both(c, carry):
        pointwise(at(jnp.maximum(c - 1, 0)), chunk)
        product(at(c), chunk)
        return carry

    lax.fori_loop(0, whole, both, 0)

    def last(rows):
        pointwise(at(jnp.maximum(whole - 1, 0)), chunk)
        product(at(whole), rows)
        pointwise(at(whole), rows)

    sized(units(tab[2, t]) - whole * per, chunk, last)


def dact_call(d_out, w_down, h_gate, h_up, table, fb, most):
    groups, _, width = d_out.shape
    ff = w_down.shape[1]
    rows = lambda tab, t: pl.ds(tab[1, t], tab[2, t])
    h_blk = ((tile_rows(most), GRP, fb), lambda tab, t, n: (rows(tab, t), 0, n))
    return piped(
        "dact",
        dact_kernel,
        lambda tab: (tab[6, 0], ff // fb),
        [table],
        [d_out, w_down, h_gate, h_up],
        [((tile_rows(most), GRP, width), lambda tab, t, n: (rows(tab, t), 0, 0)), ((1, fb, width), lambda tab, t, n: (tab[0, t], n, 0)), h_blk, h_blk],
        [jax.ShapeDtypeStruct((groups, GRP, ff), jnp.bfloat16)] * 2,
        [h_blk] * 2,
        [pltpu.VMEM((min(512, most * GRP), fb), jnp.bfloat16)],
        groups * GRP * width * ff,
        groups * GRP * ff // 2,
    )


def wgrad_kernel(tab, x_ref, d_ref, dg_ref, du_ref, act_ref, gg_ref, gu_ref, gd_ref, ag_ref, au_ref, ad_ref):
    t = pl.program_id(1)
    first, last = tab[4, t] == 1, tab[5, t] == 1
    most = x_ref.shape[0] * GRP

    def products(rows, masked):
        def load(ref):
            v = rows_of(ref, 0, rows)[...]
            if masked:
                keep = lax.broadcasted_iota(I32, (rows, ref.shape[2]), 0) < tab[3, t] * GRP
                v = jnp.where(keep, v, jnp.zeros_like(v))
            return v

        x, d = load(x_ref), load(d_ref)
        yield ag_ref, gg_ref, dot(x, load(dg_ref), 0, 0)
        yield au_ref, gu_ref, dot(x, load(du_ref), 0, 0)
        yield ad_ref, gd_ref, dot(load(act_ref), d, 0, 0)

    @pl.when(first & last)
    def _():
        for acc_ref in (ag_ref, au_ref, ad_ref):
            acc_ref[...] = jnp.zeros_like(acc_ref)

    @pl.when(~last)
    def _():
        for acc_ref, _, part in products(most, False):
            acc_ref[...] = jnp.where(first, 0.0, acc_ref[...]) + part

    def finish(rows):
        for acc_ref, out_ref, part in products(rows, True):
            out_ref[0] = (acc_ref[...] + part).astype(jnp.bfloat16)

    pairs = jnp.maximum((units(tab[3, t]) + 1) // 2, 1)
    for k in range(1, most // (2 * UNIT) + 1):
        pl.when(last & (pairs == k))(functools.partial(finish, 2 * k * UNIT))


def wgrad_call(x, d_out, d_gate, d_up, act, table, fb, most):
    groups, _, width = x.shape
    ff = act.shape[2]
    rows = lambda tab, t: pl.ds(tab[1, t], tab[2, t])
    row_in = ((tile_rows(most), GRP, width), lambda tab, n, t: (rows(tab, t), 0, 0))
    h_in = ((tile_rows(most), GRP, fb), lambda tab, n, t: (rows(tab, t), 0, n))
    up_out = ((1, width, fb), lambda tab, n, t: (tab[0, t], 0, n))
    down_out = ((1, fb, width), lambda tab, n, t: (tab[0, t], n, 0))
    up_shape = jax.ShapeDtypeStruct((2, width, ff), jnp.bfloat16)
    down_shape = jax.ShapeDtypeStruct((2, ff, width), jnp.bfloat16)
    return piped(
        "wgrad",
        wgrad_kernel,
        lambda tab: (ff // fb, tab[6, 0]),
        [table],
        [x, d_out, d_gate, d_up, act],
        [row_in, row_in, h_in, h_in, h_in],
        [up_shape, up_shape, down_shape],
        [up_out, up_out, down_out],
        [pltpu.VMEM((width, fb), jnp.float32)] * 2 + [pltpu.VMEM((fb, width), jnp.float32)],
        3 * groups * GRP * width * ff,
    )


def excl(v, axis):
    return jnp.cumsum(v, axis=axis) - v


def pair_table(starts, counts):
    return jnp.stack([jnp.arange(2, dtype=I32), starts, jnp.maximum(counts, 1), counts])


def tile_table(starts, counts, n_tiles, size, most):
    t = jnp.arange(most, dtype=I32)
    e = (t >= n_tiles[0]).astype(I32)
    of = lambda v: jnp.where(e == 0, v[0], v[1])
    i = t - e * n_tiles[0]
    have = jnp.clip(of(counts) - i * of(size), 0, of(size))
    rows = [e, of(starts) + i * of(size), jnp.maximum(have, 1), have, i == 0, i == of(n_tiles) - 1, jnp.broadcast_to(n_tiles[0] + n_tiles[1], t.shape)]
    return jnp.stack([r.astype(I32) for r in rows])


def solution(mesh):
    n_dp, n_ep = mesh.shape["dp"], mesh.shape["ep"]
    n_dev = n_dp * n_ep
    all_axes = ("dp", "ep")

    def local_step(hidden, grad_out, expert_ids, norm_gain, w_router, w_gate, w_up, w_down):
        n_tok, width = hidden.shape
        n_exp = w_router.shape[1]
        ff = w_gate.shape[2]
        capacity = 4 * n_tok // n_exp
        total_tok = n_tok * n_dev
        fb = min(512, ff)
        half = n_ep * capacity // GRP
        region = n_dp * half
        groups = 2 * region
        dp, ep = lax.axis_index("dp"), lax.axis_index("ep")
        experts = jnp.arange(n_exp, dtype=I32)
        swap = [(i, n_dp - 1 - i) for i in range(n_dp)]

        x_f32 = hidden.astype(jnp.float32)
        inv_rms = lax.rsqrt(jnp.mean(x_f32 * x_f32, axis=-1, keepdims=True) + EPS)
        x_hat = x_f32 * inv_rms
        x_norm = (x_hat * norm_gain).astype(jnp.bfloat16)
        gather = lambda v: lax.all_gather(v, "ep", axis=0, tiled=True)
        own_x = gather(x_norm)
        far_x = lax.ppermute(x_norm, "dp", swap)
        xn_f32 = x_norm.astype(jnp.float32)
        router_probs = jax.nn.softmax(jnp.dot(xn_f32, w_router, preferred_element_type=jnp.float32), axis=-1)
        choice_hot = (expert_ids[:, :, None] == experts).astype(jnp.float32)
        gate_vals = jnp.sum(router_probs[:, None, :] * choice_hot, axis=-1)

        flat_ids = expert_ids.reshape(-1)
        one_hot = (flat_ids[:, None] == experts[None, :]).astype(I32)
        running = jnp.cumsum(one_hot, axis=0) - 1
        dest_rows = flat_ids * capacity + jnp.sum(running * one_hot, axis=1)
        slots = jnp.arange(n_exp * capacity, dtype=I32)
        choices = jnp.arange(2 * n_tok, dtype=I32)
        hit = dest_rows[None, :] == slots[:, None]
        slot_tok = jnp.sum(jnp.where(hit, choices[None, :] // 2 + 1, 0), axis=1) - 1
        slot_gate = jnp.sum(jnp.where(hit, gate_vals.reshape(-1)[None, :], 0.0), axis=1)
        packed = jnp.stack([slot_tok.astype(jnp.float32), slot_gate]).reshape(2, n_exp, capacity)
        packed = lax.all_gather(packed, all_axes, axis=0, tiled=False)
        packed, late_out = lax.optimization_barrier((packed, grad_out))
        far_dy = lax.ppermute(late_out, "dp", swap)
        all_toks = packed[:, 0].astype(I32)
        all_loads = jnp.sum((all_toks >= 0).astype(I32), axis=2)
        src_groups = (all_loads + GRP - 1) // GRP
        mine = lambda v: lax.dynamic_slice_in_dim(v, 2 * ep, 2, axis=1)
        near = lambda v: lax.dynamic_slice_in_dim(v, dp * n_ep, n_ep, axis=0)
        far = lambda v: lax.dynamic_slice_in_dim(v, (n_dp - 1 - dp) * n_ep, n_ep, axis=0)
        my_groups = mine(src_groups)
        own_len, oth_len = near(my_groups), far(my_groups)
        own_off = excl(own_len, 0)
        n_own, n_oth = jnp.sum(own_len, axis=0), jnp.sum(oth_len, axis=0)
        base = jnp.arange(2, dtype=I32) * region
        n_all = n_own + n_oth
        own_tab = pair_table(base, n_own)
        oth_tab = pair_table(base + n_own, n_oth)
        split = 1 + (n_all > region * 5 // 8).astype(I32)
        all_tab = tile_table(base, n_all, split, (n_all + split - 1) // split, 4)
        k_tile = min(128, half)
        k_size = jnp.full((2,), k_tile, I32)
        k_tab = tile_table(base, n_all, jnp.maximum((n_all + k_tile - 1) // k_tile, 1), k_size, 2 * region // k_tile)
        toks, gates = mine(all_toks)[:, :, None, :], mine(packed[:, 1])[:, :, :, None]
        own = dict(slot_rows=near(toks), slot_gates=near(gates), offs=(own_off + base).reshape(-1), lens=own_len.reshape(-1), n_tok=n_tok, groups=groups)
        oth = dict(slot_rows=far(toks), slot_gates=far(gates), offs=(excl(oth_len, 0) + n_own + base).reshape(-1), lens=oth_len.reshape(-1), n_tok=n_tok, groups=groups)

        far_x, _ = lax.optimization_barrier((far_x, own_tab))
        oth_x = gather(far_x)
        x_rows = route_call("route_own", own_x, scaled=False, **own)
        first_half = up_call("up_own", x_rows, w_gate, w_up, own_tab, fb, half)
        x_rows, late_out, far_dy, *first_half = lax.optimization_barrier((x_rows, late_out, far_dy, *first_half))
        own_dy, oth_dy = gather(late_out), gather(far_dy)
        x_rows = route_call("route_oth", oth_x, scaled=False, into=[x_rows], **oth)
        h_gate, h_up, act = up_call("up_oth", x_rows, w_gate, w_up, oth_tab, fb, half, into=first_half)

        def send_back(blocks):
            return lax.all_to_all(blocks, "ep", 0, 0, tiled=True).reshape(n_exp * capacity, width)

        back_blocks = down_call("down", [act], [w_down], own_tab, own_off.T, own_len.T, capacity, fb, half)
        d_rows = route_call("droute_own", own_dy, scaled=True, **own)
        d_rows = route_call("droute_oth", oth_dy, scaled=True, into=[d_rows], **oth)
        back = send_back(back_blocks)
        d_gate, d_up = dact_call(d_rows, w_down, h_gate, h_up, all_tab, fb, region * 5 // 8)
        d_blocks = down_call("drows", [d_gate, d_up], [w_gate, w_up], own_tab, own_off.T, own_len.T, capacity, fb, half)
        back, d_blocks = lax.optimization_barrier((back, d_blocks))
        d_back = send_back(d_blocks)
        g_gate, g_up, g_down = wgrad_call(x_rows, d_rows, d_gate, d_up, act, k_tab, fb, k_tile)

        dest = dest_rows.reshape(n_tok, 2)
        pick = lambda rows, j: jnp.take(rows, dest[:, j], axis=0, mode="clip").astype(jnp.float32)
        dy_f32 = grad_out.astype(jnp.float32)
        out0, out1 = pick(back, 0), pick(back, 1)
        out_hidden = (x_f32 + (gate_vals[:, :1] * out0 + gate_vals[:, 1:] * out1)).astype(jnp.bfloat16)
        d_gates = jnp.stack([jnp.sum(dy_f32 * out0, axis=-1), jnp.sum(dy_f32 * out1, axis=-1)], axis=1)
        load_frac = jnp.sum(all_loads, axis=0).astype(jnp.float32) / (2 * total_tok)
        d_probs = jnp.sum(d_gates[:, :, None] * choice_hot, axis=1) + (AUX_COEF * n_exp / total_tok) * load_frac
        d_logits = router_probs * (d_probs - jnp.sum(router_probs * d_probs, axis=-1, keepdims=True))
        d_xnorm = jnp.einsum("te,de->td", d_logits, w_router) + pick(d_back, 0) + pick(d_back, 1)
        d_xnorm = d_xnorm.astype(jnp.bfloat16).astype(jnp.float32)
        d_hat = d_xnorm * norm_gain
        grad_hidden = (inv_rms * (d_hat - x_hat * jnp.mean(d_hat * x_hat, axis=-1, keepdims=True)) + dy_f32).astype(jnp.bfloat16)
        prob_sum, grad_gain, grad_router = lax.psum(
            (jnp.sum(router_probs, axis=0), jnp.sum(d_xnorm * x_hat, axis=0), jnp.einsum("td,te->de", xn_f32, d_logits)), all_axes
        )
        aux_loss = AUX_COEF * n_exp * jnp.sum(load_frac * prob_sum / total_tok)
        return out_hidden, aux_loss, grad_hidden, grad_gain, grad_router, g_gate, g_up, g_down

    tok_spec = P(all_axes, None)
    w_spec = P("ep", None, None)
    return jax.shard_map(
        local_step,
        mesh=mesh,
        in_specs=(tok_spec, tok_spec, tok_spec, P(), P(), w_spec, w_spec, w_spec),
        out_specs=(tok_spec, P(), tok_spec, P(), P(), w_spec, w_spec, w_spec),
        check_vma=False,
    )
```
